32 devices in a mesh: gx: 4 (over y, x), gy: 8 (over z, core).
Axes of the slice: x: 2, y: 2, z: 4, core: 2. Of those that a mesh axis runs over, the one named last changes fastest.
Arguments:
- q_nodes: bfloat16 [32, 512, 4096], P(('gx', 'gy')), may hold values from -30 to 30, as said below
- k_cache: bfloat16 [32, 1024, 512], P(('gx', 'gy')), may hold values from -6 to 6, as said below
- v_cache: bfloat16 [32, 1024, 512], P(('gx', 'gy')), may hold values from -6 to 6
- k_tree: bfloat16 [32, 512, 512], P(('gx', 'gy')), may hold values from -6 to 6
- v_tree: bfloat16 [32, 512, 512], P(('gx', 'gy')), may hold values from -6 to 6
- anc_bits: int32 [32, 512, 16], P(('gx', 'gy')), may hold values from -2147483648 to 2147483647, as said below
- node_count: int32 [32], P(('gx', 'gy')), may hold values from 1 to 512, as said below
- cache_len: int32 [32], P(('gx', 'gy')), may hold values from 256 to 1024, as said below
- sinks: float32 [64], replicated, may hold values from 5 to 10
- o_weight: bfloat16 [4096, 2880], P(('gx', 'gy')), may hold values from -0.09375 to 0.09375
Outputs:
- attended: bfloat16 [32, 512, 4096], P(('gx', 'gy'))
- projected: bfloat16 [32, 512, 2880], P(('gx', 'gy'))
The draws below stay inside these ranges and needn't reach their ends.
Inputs may be any that keep to these rules, and one draw needn't show every extreme that they name: `q_nodes`: custom draw of queries. `k_cache`: custom draw of keys. `anc_bits`: bit j mod 32 of word j // 32 in row i is set exactly when tree node j is node i or one of its ancestors; node 0 is the root and a node's ancestors have lower indices. `node_count`: write request r as a * 8 + b with b < 8. Where a + b is even, the tree has more than (2) * 128 nodes; elsewhere it has at most 128. Request 0 has 512 nodes. `cache_len`: request 0 has 1024 cached positions.
All inputs are finite; a program needn't handle non-finite values.
Results may differ from the reference program's by a relative error of at most 0.0055.
Values may be sent and summed in bfloat16 or wider, within the bound.
A program may use at most 192 MiB of HBM per device.

```python
import jax
import jax.numpy as jnp
from jax import lax

QH = 64
KVH = 8
HD = 64
D = 2880
TREE_MAX = 512
BLK = 128
CACHE_MAX = 1024
REQUESTS = 32
N_GY = 8


def tree_tables(key):
    base_key = jax.random.fold_in(key, 11)
    block_count = TREE_MAX // BLK
    request_ids = jnp.arange(REQUESTS, dtype=jnp.int32)
    parity = (request_ids // N_GY + request_ids % N_GY) % 2
    busy_blocks = jax.random.randint(jax.random.fold_in(base_key, 1), (REQUESTS,), block_count - 1, block_count + 1)
    live_blocks = jnp.where(parity == 0, busy_blocks, 1).astype(jnp.int32)
    extra_nodes = jax.random.randint(jax.random.fold_in(base_key, 2), (REQUESTS,), 1, BLK + 1)
    node_total = ((live_blocks - 1) * BLK + extra_nodes).astype(jnp.int32)
    node_total = node_total.at[0].set(TREE_MAX)
    steps_back = jax.random.randint(jax.random.fold_in(base_key, 3), (REQUESTS, TREE_MAX), 1, 5)
    parents = jnp.maximum(jnp.arange(TREE_MAX, dtype=jnp.int32)[None, :] - steps_back, 0).astype(jnp.int32)
    word_count = TREE_MAX // 32
    word_ids = jnp.arange(word_count, dtype=jnp.int32)
    row_ids = jnp.arange(REQUESTS, dtype=jnp.int32)

    def add_node(node_index, bit_table):
        parent_row = bit_table[row_ids, parents[:, node_index]]
        parent_row = jnp.where(node_index > 0, parent_row, jnp.zeros_like(parent_row))
        own_bit = jnp.where(word_ids == node_index // 32, jnp.left_shift(jnp.asarray(1, jnp.int32), node_index % 32), 0).astype(jnp.int32)
        new_row = jnp.bitwise_or(parent_row, own_bit[None, :])
        return lax.dynamic_update_slice(bit_table, new_row[:, None, :], (0, node_index, 0))
    bit_table = lax.fori_loop(0, TREE_MAX, add_node, jnp.zeros((REQUESTS, TREE_MAX, word_count), jnp.int32))
    return (node_total, bit_table)


def draw_node_count(key, part):
    return tree_tables(key)[0]


def draw_anc_bits(key, part):
    return tree_tables(key)[1]


def draw_cache_len(key, part):
    counts = jax.random.randint(jax.random.fold_in(key, 41), (REQUESTS,), CACHE_MAX // 4, CACHE_MAX + 1)
    return counts.astype(jnp.int32).at[0].set(CACHE_MAX)


def draw_k_cache(key, part):
    full_shape = (REQUESTS, CACHE_MAX, KVH * HD)
    values = jnp.clip(jax.random.normal(jax.random.fold_in(key, 21), full_shape, jnp.float32), -6.0, 6.0)
    return values.astype(jnp.bfloat16)


def draw_q_nodes(key, part):
    full_shape = (REQUESTS, TREE_MAX, QH * HD)
    values = jnp.clip(2.0 * jax.random.normal(jax.random.fold_in(key, 31), full_shape, jnp.float32), -12.0, 12.0)
    return values.astype(jnp.bfloat16)


def steps_of(rng, dims, split, smallest, largest):
    gain, own = 1.0, jax.random.fold_in(rng, 6)
    for position, blocks in split:
        steps = jnp.exp(jax.random.uniform(jax.random.fold_in(own, position), (blocks,), jnp.float32, smallest / len(split), largest / len(split)))
        gain = gain * jnp.repeat(steps, dims[position] // blocks).reshape([-1 if axis == position else 1 for axis in range(len(dims))])
    return gain


def bell_draw(key, extent, spread, most, cuts=(), kind=jnp.bfloat16):
    drawn = spread * jax.random.normal(key, extent, jnp.float32)
    if cuts:
        drawn = drawn * steps_of(key, extent, cuts, -0.22, 0.18)
    return jnp.clip(drawn, -most, most).astype(kind)


def setup_inputs(seed: int = 0) -> dict:
    keys = jax.random.split(jax.random.key(seed), 11)
    q_nodes = draw_q_nodes(jax.random.fold_in(keys[10], 71), 0)
    k_cache = draw_k_cache(jax.random.fold_in(keys[10], 71), 0)
    v_cache = bell_draw(keys[2], (REQUESTS, CACHE_MAX, KVH * HD), 1.0, 6.0, ((0, 32),))
    k_tree = bell_draw(keys[3], (REQUESTS, TREE_MAX, KVH * HD), 1.0, 6.0, ((0, 32),))
    v_tree = bell_draw(keys[4], (REQUESTS, TREE_MAX, KVH * HD), 1.0, 6.0, ((0, 32),))
    anc_bits = draw_anc_bits(jax.random.fold_in(keys[10], 71), 0)
    node_count = draw_node_count(jax.random.fold_in(keys[10], 71), 0)
    cache_len = draw_cache_len(jax.random.fold_in(keys[10], 71), 0)
    sinks = jnp.clip(jax.random.uniform(keys[8], (QH,), jnp.float32, 5.0, 10.0), 5.0, 10.0)
    o_weight = bell_draw(keys[9], (QH * HD, D), (QH * HD) ** -0.5, 0.09375, ((0, 32),))
    return dict(q_nodes=q_nodes, k_cache=k_cache, v_cache=v_cache, k_tree=k_tree, v_tree=v_tree, anc_bits=anc_bits, node_count=node_count, cache_len=cache_len, sinks=sinks, o_weight=o_weight)


MASKED = -1.0e30


def unpack_bits(bit_words):
    shift_ids = jnp.arange(32, dtype=jnp.int32)
    bit_flags = jnp.bitwise_and(jnp.right_shift(bit_words[:, :, None], shift_ids), 1)
    return bit_flags.reshape(bit_words.shape[0], bit_words.shape[1] * 32) > 0


def attend_rows(q_rows, tree_ok, cache_keys, cache_values, tree_keys, tree_values, cache_count, sinks):
    row_total = q_rows.shape[0]
    groups = QH // KVH
    head_width = groups * HD
    scale_factor = HD ** -0.5
    cache_ok = jnp.arange(cache_keys.shape[0], dtype=jnp.int32) < cache_count
    tree_mask = jnp.repeat(tree_ok, groups, axis=0)

    def per_kv_head(kv_head):
        q_part = lax.dynamic_slice_in_dim(q_rows, kv_head * head_width, head_width, 1).reshape(row_total * groups, HD)
        key_cache = lax.dynamic_slice_in_dim(cache_keys, kv_head * HD, HD, 1)
        value_cache = lax.dynamic_slice_in_dim(cache_values, kv_head * HD, HD, 1)
        key_tree = lax.dynamic_slice_in_dim(tree_keys, kv_head * HD, HD, 1)
        value_tree = lax.dynamic_slice_in_dim(tree_values, kv_head * HD, HD, 1)
        score_cache = jnp.dot(q_part, key_cache.T, preferred_element_type=jnp.float32) * scale_factor
        score_cache = jnp.where(cache_ok[None, :], score_cache, MASKED)
        score_tree = jnp.dot(q_part, key_tree.T, preferred_element_type=jnp.float32) * scale_factor
        score_tree = jnp.where(tree_mask, score_tree, MASKED)
        sink_rows = jnp.tile(lax.dynamic_slice_in_dim(sinks, kv_head * groups, groups, 0), row_total)
        row_max = jnp.maximum(sink_rows, jnp.maximum(jnp.max(score_cache, axis=1), jnp.max(score_tree, axis=1)))
        weight_cache = jnp.exp(score_cache - row_max[:, None])
        weight_tree = jnp.exp(score_tree - row_max[:, None])
        denominator = jnp.exp(sink_rows - row_max) + jnp.sum(weight_cache, axis=1) + jnp.sum(weight_tree, axis=1)
        numerator = jnp.dot(weight_cache.astype(jnp.bfloat16), value_cache, preferred_element_type=jnp.float32)
        numerator = numerator + jnp.dot(weight_tree.astype(jnp.bfloat16), value_tree, preferred_element_type=jnp.float32)
        return (numerator / denominator[:, None]).reshape(row_total, head_width)

    per_head = lax.map(per_kv_head, jnp.arange(KVH, dtype=jnp.int32))
    return jnp.transpose(per_head, (1, 0, 2)).reshape(row_total, QH * HD)


def reference(q_nodes, k_cache, v_cache, k_tree, v_tree, anc_bits, node_count, cache_len, sinks, o_weight):
    def per_request(request):
        queries, cache_keys, cache_values, tree_keys, tree_values, bit_words, node_limit, cache_count = request
        result = attend_rows(queries, unpack_bits(bit_words), cache_keys, cache_values, tree_keys, tree_values, cache_count, sinks)
        node_live = jnp.arange(queries.shape[0], dtype=jnp.int32) < node_limit
        attended_rows = jnp.where(node_live[:, None], result, jnp.zeros_like(result)).astype(jnp.bfloat16)
        projected_rows = jnp.dot(attended_rows, o_weight, preferred_element_type=jnp.float32).astype(jnp.bfloat16)
        return attended_rows, projected_rows

    attended, projected = lax.map(per_request, (q_nodes, k_cache, v_cache, k_tree, v_tree, anc_bits, node_count, cache_len))
    return (attended, projected)
```

```python
import functools

import jax
import jax.numpy as jnp
from jax import lax
from jax.experimental import pallas as pl
from jax.experimental.pallas import tpu as pltpu
from jax.sharding import PartitionSpec as P

QH = 64
KVH = 8
HD = 64
BLK = 128
PAIRS = QH // KVH // 2
MASKED = -1e30
MESH = pl.DeviceIdType.MESH


def gray(r, size):
    out, bit = 0, 1
    while bit < size:
        out = out + ((r // bit) % 2 + (r // (2 * bit)) % 2) % 2 * bit
        bit *= 2
    return out


def ungray(g, size):
    out, bit = 0, 1
    while bit < size:
        total, top = 0, bit
        while top < size:
            total = total + (g // top) % 2
            top *= 2
        out = out + total % 2 * bit
        bit *= 2
    return out


def kernel(
    R, L,
    q_h, kc_h, vc_h, kt_h, vt_h, bits_ref, nc_ref, cl_ref, sinks_ref, w_h,
    att_h, proj_h, wfull,
    w_own, q_v, k_v, v_v, kk, vv, bias, att_v, acc, wbuf, proj_v,
    line_send, line_recv, ring_send, ring_recv, d2d_send, d2d_recv, load_sem, wb_sem, own_sem, out_sem,
):
    gx, gy = lax.axis_index("gx"), lax.axis_index("gy")
    core, z = gy % 2, gy // 2
    r = ungray(gx, R)
    rows = w_own.shape[0]
    half = rows // 2
    nodes = q_v.shape[0]
    cache = kc_h.shape[0]
    busy = (gx + gy) % 2 == 0

    def dev(rr, zz, cc):
        return (gray(rr % R, R), 2 * zz + cc)

    def row_of(rr, zz, cc, h=0):
        return pl.multiple_of((gray(rr % R, R) * 2 * L + 2 * zz + cc) * rows + h * half, 16)

    right, left = dev(r + 1, z, core), dev(r + R - 1, z, core)
    partner = (gx, 2 * z + 1 - core)

    barrier = pltpu.get_barrier_semaphore()
    for nb in (right, left, partner):
        pl.semaphore_signal(barrier, inc=1, device_id=nb, device_id_type=MESH)

    @pl.when(z > 0)
    def _():
        pl.semaphore_signal(barrier, inc=1, device_id=(gx, gy - 2), device_id_type=MESH)

    @pl.when(z < L - 1)
    def _():
        pl.semaphore_signal(barrier, inc=1, device_id=(gx, gy + 2), device_id_type=MESH)

    own_load = pltpu.make_async_copy(w_h, w_own, own_sem.at[0])
    own_load.start()
    loads = [
        pltpu.make_async_copy(q_h, q_v, load_sem.at[0]),
        pltpu.make_async_copy(kc_h, k_v.at[pl.ds(0, cache)], load_sem.at[1]),
        pltpu.make_async_copy(vc_h, v_v.at[pl.ds(0, cache)], load_sem.at[2]),
        pltpu.make_async_copy(kt_h, k_v.at[pl.ds(cache, nodes)], load_sem.at[3]),
        pltpu.make_async_copy(vt_h, v_v.at[pl.ds(cache, nodes)], load_sem.at[4]),
    ]
    for c in loads:
        c.start()
    pl.semaphore_wait(barrier, 3 + jnp.minimum(z, 1) + jnp.minimum(L - 1 - z, 1))
    own_load.wait()

    def piece(rr, zz, cc, h):
        return wfull.at[pl.ds(row_of(rr, zz, cc, h), half)]

    def line_copy(src, zz, up):
        d = 0 if up else 1
        return pltpu.make_async_remote_copy(
            src_ref=src, dst_ref=wfull.at[pl.ds(row_of(r, zz, core), rows)],
            send_sem=line_send.at[d, zz], recv_sem=line_recv.at[zz],
            device_id=(gx, gy + 2 if up else gy - 2), device_id_type=MESH,
        )

    def ring_copy(src, rr, zz, h):
        return pltpu.make_async_remote_copy(
            src_ref=src, dst_ref=piece(rr, zz, core, h),
            send_sem=ring_send.at[h, rr, zz], recv_sem=ring_recv.at[h, rr, zz],
            device_id=left if h else right, device_id_type=MESH,
        )

    def d2d_copy(src, rr, zz, h, cc=None):
        return pltpu.make_async_remote_copy(
            src_ref=src, dst_ref=piece(rr, zz, core if cc is None else cc, h),
            send_sem=d2d_send.at[h, rr, zz], recv_sem=d2d_recv.at[h, rr, zz],
            device_id=partner, device_id_type=MESH,
        )

    @pl.when(z < L - 1)
    def _():
        line_copy(w_own, z, True).start()

    @pl.when(z > 0)
    def _():
        line_copy(w_own, z, False).start()

    for h in range(2):
        ring_copy(w_own.at[pl.ds(h * half, half)], r, z, h).start()
    for h in range(2):
        d2d_copy(w_own.at[pl.ds(h * half, half)], r, z, h).start()
    own_store = pltpu.make_async_copy(w_own, wfull.at[pl.ds(row_of(r, z, core), rows)], own_sem.at[1])
    own_store.start()

    def z_at(t):
        m = jnp.minimum(z, L - 1 - z)
        k = (t + 1) // 2
        near = z + k * (2 * (t % 2) - 1)
        far = jnp.where(z < L - 1 - z, z + t - m, z - t + m)
        return jnp.where(t <= 2 * m, near, far)

    def line_event(t):
        zz = z_at(t)
        share = wfull.at[pl.ds(row_of(r, zz, core), rows)]
        line_copy(share, zz, True).wait_recv()

        @pl.when(jnp.logical_and(zz < z, z < L - 1))
        def _():
            line_copy(share, zz, True).start()

        @pl.when(jnp.logical_and(zz > z, z > 0))
        def _():
            line_copy(share, zz, False).start()

        for h in range(2):
            ring_copy(piece(r, zz, core, h), r, zz, h).start()
        for h in range(2):
            d2d_copy(piece(r, zz, core, h), r, zz, h).start()

    def service(e):
        t = e // (R - 1)
        j = e % (R - 1) + 1

        @pl.when(jnp.logical_and(j == min(2, R - 1), t + 1 < L))
        def _():
            line_event(t + 1)

        zz = z_at(t)
        for h in range(2):
            rr = (r + j if h else r + R - j) % R
            here = piece(rr, zz, core, h)
            ring_copy(here, rr, zz, h).wait_recv()

            @pl.when(j < R - 1)
            def _():
                ring_copy(here, rr, zz, h).start()

            d2d_copy(here, rr, zz, h).start()

    events = L * (R - 1)

    lane = lax.broadcasted_iota(jnp.int32, (nodes, 128), 1)
    for t in range(nodes // 128):
        word = bits_ref[:, 4 * t + 3 : 4 * t + 4]
        for w in (2, 1, 0):
            word = jnp.where(lane < 32 * (w + 1), bits_ref[:, 4 * t + w : 4 * t + w + 1], word)
        flag = jnp.bitwise_and(jnp.right_shift(word, lane % 32), 1)
        bias[:, t * 128 : (t + 1) * 128] = jnp.where(flag > 0, 0.0, MASKED).astype(jnp.float32)

    @pl.when(jnp.logical_not(busy))
    def _():
        att_v[...] = jnp.zeros_like(att_v)

    for c in loads:
        c.wait()

    total = cache + nodes
    key_id = lax.broadcasted_iota(jnp.int32, (total, 128), 0)
    key_ok = jnp.logical_or(key_id < cl_ref[0], key_id >= cache)
    low = lax.broadcasted_iota(jnp.int32, (total, 128), 1) < HD
    ones = jnp.where(key_ok, 1.0, 0.0)
    vv[0, :, 128:] = jnp.where(low, ones, 0.0).astype(jnp.bfloat16)
    vv[1, :, 128:] = jnp.where(low, 0.0, ones).astype(jnp.bfloat16)

    def prepare(g):
        col = pl.ds(pl.multiple_of(g // 2 * 128, 128), 128)
        for src, dst, gain in ((k_v, kk, HD**-0.5), (v_v, vv, 1.0)):
            x = src[:, col].astype(jnp.float32) * gain
            x = jnp.where(key_ok, x, 0.0)
            y = pltpu.roll(x, HD, 1)
            even = (g + jnp.zeros_like(key_id)) % 2 == 0
            dst[0, :, :128] = jnp.where(low, jnp.where(even, x, y), 0.0).astype(jnp.bfloat16)
            dst[1, :, :128] = jnp.where(low, 0.0, jnp.where(even, y, x)).astype(jnp.bfloat16)

    def unit(g, i):
        first = i * BLK
        keys = cache + first + BLK
        qs = jnp.concatenate(
            [
                q_v[first : first + BLK, pl.ds(pl.multiple_of(g * 2 * PAIRS * HD + p * 128, 128), 128)]
                for p in range(PAIRS)
            ],
            axis=0,
        )
        mask = bias[first : first + BLK, : first + BLK]
        mask = jnp.concatenate([mask] * PAIRS, axis=0)
        out, extra = None, []
        for h in range(2):
            s = lax.dot_general(
                qs, kk[h, :keys, :], (((1,), (1,)), ((), ())), preferred_element_type=jnp.float32
            )
            s_tree = s[:, cache:] + mask
            s_cache = s[:, :cache]
            sink = jnp.concatenate(
                [jnp.full((BLK, 1), sinks_ref[g * 2 * PAIRS + 2 * p + h], jnp.float32) for p in range(PAIRS)],
                axis=0,
            )
            top = jnp.maximum(
                sink,
                jnp.maximum(
                    jnp.max(s_cache, axis=1, keepdims=True), jnp.max(s_tree, axis=1, keepdims=True)
                ),
            )
            p_cache = jnp.exp(s_cache - top).astype(jnp.bfloat16)
            p_tree = jnp.exp(s_tree - top).astype(jnp.bfloat16)
            o = jnp.dot(p_cache, vv[h, :cache, :], preferred_element_type=jnp.float32)
            o = o + jnp.dot(p_tree, vv[h, cache:keys, :], preferred_element_type=jnp.float32)
            out = o if out is None else out + o
            extra.append(jnp.exp(sink - top))
        lanes = lax.broadcasted_iota(jnp.int32, (PAIRS * BLK, 128), 1)
        den = out[:, 128:] + jnp.where(lanes < HD, extra[0], extra[1])
        res = out[:, :128] / den
        row = lax.broadcasted_iota(jnp.int32, (BLK, 128), 0) + first
        for p in range(PAIRS):
            part = jnp.where(row < nc_ref[0], res[p * BLK : (p + 1) * BLK], 0.0)
            att_v[
                first : first + BLK, pl.ds(pl.multiple_of(g * 2 * PAIRS * HD + p * 128, 128), 128)
            ] = part.astype(jnp.bfloat16)

    early = min(KVH, events)

    def head_step(g, carry):
        prepare(g)
        unit(g, 0)

        @pl.when(busy)
        def _():
            for i in range(1, nodes // BLK):
                unit(g, i)

        @pl.when(g < early)
        def _():
            service(g)

        return carry

    lax.fori_loop(0, KVH, head_step, 0)
    att_store = pltpu.make_async_copy(att_v, att_h, out_sem.at[0])
    att_store.start()
    own_store.wait()
    acc[...] = jnp.zeros_like(acc)

    def chunk_load(rr, zz):
        return pltpu.make_async_copy(
            wfull.at[pl.ds(row_of(rr, zz, 0), 2 * rows)], wbuf.at[rr % 2], wb_sem.at[rr % 2]
        )

    def project(t):
        zz = z_at(t)
        for h in range(2):
            for rr in range(R):
                d2d_copy(piece(rr, zz, core, h), rr, zz, h, 1 - core).wait_recv()
        chunk_load(0, zz).start()
        for rr in range(R):
            if rr + 1 < R:
                chunk_load(rr + 1, zz).start()
            chunk_load(rr, zz).wait()
            a = att_v[:, pl.ds(row_of(rr, zz, 0), 2 * rows)] if (2 * rows) % 128 == 0 else None
            if a is None:
                base = row_of(rr, zz, 0)
                wide = att_v[:, pl.ds(pl.multiple_of(base // 128 * 128, 128), 128)]
                col = lax.broadcasted_iota(jnp.int32, (128, 2 * rows), 0)
                pick = col == base % 128 + lax.broadcasted_iota(jnp.int32, (128, 2 * rows), 1)
                a = jnp.dot(
                    wide, jnp.where(pick, 1.0, 0.0).astype(jnp.bfloat16), preferred_element_type=jnp.float32
                ).astype(jnp.bfloat16)
            acc[...] += jnp.dot(a, wbuf[rr % 2], preferred_element_type=jnp.float32)

    def project_step(t, carry):
        def late(e, c):
            service(e)
            return c

        lax.fori_loop(jnp.maximum(t * (R - 1), early), jnp.maximum((t + 1) * (R - 1), early), late, 0)
        project(t)
        return carry

    lax.fori_loop(0, L, project_step, 0)
    proj_v[...] = acc[...].astype(jnp.bfloat16)
    proj_store = pltpu.make_async_copy(proj_v, proj_h, out_sem.at[1])
    proj_store.start()

    def drain(zz, carry):
        @pl.when(jnp.logical_and(zz <= z, z < L - 1))
        def _():
            line_copy(w_own, zz, True).wait_send()

        @pl.when(jnp.logical_and(zz >= z, z > 0))
        def _():
            line_copy(w_own, zz, False).wait_send()

        for h in range(2):
            for j in range(R - 1):
                rr = (r + j if h else r + R - j) % R
                ring_copy(piece(rr, zz, core, h), rr, zz, h).wait_send()
            for rr in range(R):
                d2d_copy(piece(rr, zz, core, h), rr, zz, h).wait_send()
        return carry

    lax.fori_loop(0, L, drain, 0)
    att_store.wait()
    proj_store.wait()


def solution(mesh):
    R, L = mesh.shape["gx"], mesh.shape["gy"] // 2

    def on_device(q, kc, vc, kt, vt, bits, nc, cl, sinks, w):
        nodes, width = q.shape[1:]
        cache, kvw = kc.shape[1:]
        rows, d = w.shape
        total = cache + nodes
        bf, f32 = jnp.bfloat16, jnp.float32
        hbm = pl.BlockSpec(memory_space=pl.ANY)
        smem = pl.BlockSpec(memory_space=pltpu.SMEM)
        dma = pltpu.SemaphoreType.DMA
        att, proj, _ = pl.pallas_call(
            functools.partial(kernel, R, L),
            out_shape=(
                jax.ShapeDtypeStruct((nodes, width), bf),
                jax.ShapeDtypeStruct((nodes, d), bf),
                jax.ShapeDtypeStruct((width, d), bf),
            ),
            in_specs=[hbm] * 5 + [pl.BlockSpec(memory_space=pltpu.VMEM), smem, smem, smem, hbm],
            out_specs=(hbm, hbm, hbm),
            scratch_shapes=[
                pltpu.VMEM((rows, d), bf),
                pltpu.VMEM((nodes, width), bf),
                pltpu.VMEM((total, kvw), bf),
                pltpu.VMEM((total, kvw), bf),
                pltpu.VMEM((2, total, 128), bf),
                pltpu.VMEM((2, total, 256), bf),
                pltpu.VMEM((nodes, nodes), f32),
                pltpu.VMEM((nodes, width), bf),
                pltpu.VMEM((nodes, d), f32),
                pltpu.VMEM((2, 2 * rows, d), bf),
                pltpu.VMEM((nodes, d), bf),
                dma((2, L)), dma((L,)), dma((2, R, L)), dma((2, R, L)), dma((2, R, L)), dma((2, R, L)),
                dma((5,)), dma((2,)), dma((2,)), dma((2,)),
            ],
            compiler_params=pltpu.CompilerParams(
                collective_id=0, has_side_effects=True, vmem_limit_bytes=60 * 1024 * 1024
            ),
        )(q[0], kc[0], vc[0], kt[0], vt[0], bits[0], nc, cl, sinks, w)
        return att[None], proj[None]

    both = ("gx", "gy")
    cube = P(both, None, None)
    return jax.shard_map(
        on_device,
        mesh=mesh,
        in_specs=(cube,) * 6 + (P(both), P(both), P(), P(both, None)),
        out_specs=(cube, cube),
        check_vma=False,
    )
```
